256 devices in a mesh: tm: 128 (over z_lo, x, y, core), chan: 2 (over z_hi).
Axes of the slice: x: 4, y: 4, z: 8 (z_hi: 2, z_lo: 4; z = z_hi * 4 + z_lo), core: 2. Of those that a mesh axis runs over, the one named last changes fastest.
Arguments:
- spectrum: float32 [256, 131072], P('tm', 'chan'), may hold values from -6 to 6
- offsets: int32 [512], replicated, may hold values from 0 to 128, as said below
Outputs:
- peak: float32 [131072], P('chan')
The draws below stay inside these ranges and needn't reach their ends.
Inputs may be any that keep to these rules, and one draw needn't show every extreme that they name: `offsets`: entries 0 and 1 are 0; entry 2L + d (drift d of the section that joins blocks of L) lies in 0 to L, and is exactly L for d = 2L - 1.
All inputs are finite; a program needn't handle non-finite values.
Results may differ from the reference program's by a relative error of at most 0.00002.
Values sent between devices are 32-bit elements; how exact they have to be, the bound alone decides.
No kernel may reach another device: no remote copies, remote signals or barrier semaphores. Data moves between devices by JAX's collectives and lax.ppermute only.
A program may use at most 64 MiB of HBM per device.

```python
import jax
import jax.numpy as jnp
from jax import lax

TOTAL = 256
CHANNELS = 131072


def draw_offsets(key, part):
    count = 2 * TOTAL
    places = jnp.arange(count, dtype=jnp.int32)
    section = jnp.where(places >= 2, 1, 0).astype(jnp.int32)
    for power in range(1, 24):
        section = jnp.where(places >= 2 ** (power + 1), 2 ** power, section).astype(jnp.int32)
    drift = places - 2 * section
    jitter = jax.random.randint(jax.random.fold_in(key, 7), (count,), -1, 2).astype(jnp.int32)
    value = jnp.clip((drift + 1) // 2 + jitter, 0, section)
    value = jnp.where(drift == 2 * section - 1, section, value)
    value = jnp.where(places < 2, 0, value)
    return value.astype(jnp.int32)


def shard_levels(rng, shape, split, low, high):
    def one(axis_at, shards_of):
        draws = jax.random.uniform(jax.random.fold_in(jax.random.fold_in(rng, 6), axis_at), (shards_of,), jnp.float32, low / len(split), high / len(split))
        return jnp.repeat(jnp.exp(draws), shape[axis_at] // shards_of).reshape((-1,) + (1,) * (len(shape) - axis_at - 1))

    loudness = one(*split[0])
    for cut in split[1:]:
        loudness = loudness * one(*cut)
    return loudness


def noise(stream_key, extent, deviation, limit, cuts=(), kind=jnp.bfloat16):
    values = jax.random.normal(stream_key, extent, jnp.float32) * deviation
    if len(cuts) > 0:
        values = shard_levels(stream_key, extent, cuts, -0.22, 0.18) * values
    return jnp.clip(values, min=-limit, max=limit).astype(kind)


def setup_inputs(seed: int = 0) -> dict:
    splits = jax.random.split(jax.random.key(seed), 3)
    spectrum = noise(splits[0], (TOTAL, CHANNELS), 1.0, 6.0, ((0, 128), (1, 2)), jnp.float32)
    offsets = draw_offsets(jax.random.fold_in(splits[2], 71), 0)
    return {"spectrum": spectrum, "offsets": offsets}


def take_window(single, amount, span_cols):
    return lax.dynamic_slice_in_dim(single, amount, span_cols)


def combine(lower_rows, upper_ext, shifts, span_cols):
    upper_two = jnp.repeat(upper_ext, 2, axis=0)
    moved = jax.vmap(take_window, in_axes=(0, 0, None))(upper_two, shifts, span_cols)
    return jnp.repeat(lower_rows[:, :span_cols], 2, axis=0) + moved


def reference(spectrum, offsets):
    total = spectrum.shape[0]
    channels = spectrum.shape[1]
    sums = spectrum
    length = 1
    while length < total:
        blocks = total // (2 * length)
        paired = sums.reshape(blocks, 2, length, channels)
        lower_rows = paired[:, 0].reshape(blocks * length, channels)
        upper_rows = paired[:, 1].reshape(blocks * length, channels)
        upper_ext = jnp.pad(upper_rows, ((0, 0), (0, length)))
        shifts = jnp.tile(offsets[2 * length:4 * length], blocks).astype(jnp.int32)
        sums = combine(lower_rows, upper_ext, shifts, channels)
        length = length * 2
    return jnp.max(sums, axis=0)
```

```python
import functools

import jax
import jax.numpy as jnp
from jax import lax
from jax.experimental import pallas as pl
from jax.experimental.pallas import tpu as pltpu
from jax.sharding import PartitionSpec as P

LANES = 128


def tree_kernel(total, cols, halo_cols, copies, offs_ref, main_ref, halo_ref, out_ref, a_ref, b_ref):
    lane = lax.broadcasted_iota(jnp.int32, (8, LANES), 1)
    pairs = total // 2
    tail = jnp.zeros((8 - cols - halo_cols, LANES), jnp.float32)

    def fetch(i, _):
        t = i // 2
        r = i % 2
        head = main_ref[pl.ds(t * (2 * cols) + r, cols, stride=2), :]
        more = halo_ref[pl.ds(t * (2 * halo_cols) + r, halo_cols, stride=2), :]
        a_ref[i] = jnp.concatenate([head, more, tail], axis=0)
        return _

    lax.fori_loop(0, total, fetch, 0, unroll=8)

    def moved(upper, amount):
        turned = pltpu.roll(upper, (LANES - amount) & (LANES - 1), axis=1)
        return jnp.where(lane < LANES - amount, turned, pltpu.roll(turned, 7, axis=0))

    src, dst = a_ref, b_ref
    length = 1
    while length < total // 2:
        blocks = total // (2 * length)

        def level(k, _, src=src, dst=dst, length=length, blocks=blocks):
            p = k // blocks
            b = k % blocks
            lower = src[2 * b * length + p]
            upper = src[(2 * b + 1) * length + p]
            for odd in range(2):
                d = 2 * p + odd
                amount = offs_ref[2 * length + d]
                dst[b * 2 * length + d] = lower + moved(upper, amount)
            return _

        lax.fori_loop(0, pairs, level, 0, unroll=8)
        src, dst = dst, src
        length *= 2

    def last(p, best):
        lower = src[p]
        upper = src[length + p]
        for odd in range(2):
            amount = offs_ref[2 * length + 2 * p + odd]
            best = jnp.maximum(best, lower + moved(upper, amount))
        return best

    best = lax.fori_loop(0, length, last, jnp.full((8, LANES), -jnp.inf, jnp.float32), unroll=8)
    for k in range(copies):
        out_ref[pl.ds(k * cols, cols), :] = best[:cols]


def to_previous(count, groups):
    place = [q % count * groups + q // count for q in range(count * groups)]
    return list(zip(place[1:], place))


def local(spectrum, offsets):
    rows, span = spectrum.shape
    count = lax.axis_size("tm")
    groups = lax.axis_size("chan")
    total = rows * count
    cols = span // count // LANES
    halo_cols = -(-(total - 1) // LANES)
    tiles = spectrum.reshape(rows, span // LANES, LANES).transpose(1, 0, 2)
    main = lax.all_to_all(tiles, "tm", 0, 0, tiled=True)
    edge = main.reshape(count, cols, rows, LANES)[:, :halo_cols]
    halo = lax.ppermute(edge, ("tm", "chan"), to_previous(count, groups))
    best = pl.pallas_call(
        functools.partial(tree_kernel, total, cols, halo_cols, count),
        out_shape=jax.ShapeDtypeStruct((count * cols, LANES), jnp.float32),
        in_specs=[
            pl.BlockSpec(memory_space=pltpu.SMEM),
            pl.BlockSpec(memory_space=pltpu.VMEM),
            pl.BlockSpec(memory_space=pltpu.VMEM),
        ],
        out_specs=pl.BlockSpec(memory_space=pltpu.VMEM),
        scratch_shapes=[pltpu.VMEM((total, 8, LANES), jnp.float32)] * 2,
    )(offsets, main.reshape(-1, LANES), halo.reshape(-1, LANES))
    peak = lax.all_to_all(best, "tm", 0, 0, tiled=True)
    return peak.reshape(span)


def solution(mesh):
    placed = (P("tm", "chan"), P())
    return jax.shard_map(local, mesh=mesh, in_specs=placed, out_specs=P("chan"), check_vma=False)
```

```python
import functools

import jax
import jax.numpy as jnp
from jax import lax
from jax.experimental import pallas as pl
from jax.experimental.pallas import tpu as pltpu
from jax.sharding import PartitionSpec as P

LANES = 128
VMEM_LIMIT = 6 * 2**20


def sublanes():
    return lax.broadcasted_iota(jnp.int32, (8, LANES), 0)


def moved(upper, amount):
    lane = lax.broadcasted_iota(jnp.int32, (8, LANES), 1)
    turned = pltpu.roll(upper, (LANES - amount) & (LANES - 1), axis=1)
    return jnp.where(lane < LANES - amount, turned, pltpu.roll(turned, 7, axis=0))


def tree(offs_ref, get, total, a_ref, b_ref):
    half = total // 2
    for q in range(half // 2):
        lower, upper = get(q, 0), get(q, 1)
        for d in range(2):
            b_ref[2 * q + d] = lower + moved(upper, offs_ref[2 + d])
    src, dst = b_ref, a_ref
    length = 2
    while length < half:
        for p in range(length):
            amounts = [offs_ref[2 * length + 2 * p + odd] for odd in range(2)]
            for b in range(half // (2 * length)):
                lower = src[2 * b * length + p]
                upper = src[(2 * b + 1) * length + p]
                for odd in range(2):
                    dst[b * 2 * length + 2 * p + odd] = lower + moved(upper, amounts[odd])
        src, dst = dst, src
        length *= 2
    first = sublanes() < 4
    best = [jnp.full((8, LANES), -jnp.inf, jnp.float32) for _ in range(4)]
    for p in range(half):
        both = src[p]
        other = pltpu.roll(both, 4, axis=0)
        lower = jnp.where(first, both, other)
        even = moved(other, offs_ref[2 * length + 2 * p])
        odd = moved(both, offs_ref[2 * length + 2 * p + 1])
        best[p % 4] = jnp.maximum(best[p % 4], lower + jnp.where(first, even, odd))
    peak = functools.reduce(jnp.maximum, best)
    return jnp.maximum(peak, pltpu.roll(peak, 4, axis=0))


def near_kernel(total, offs_ref, main_ref, out_ref, a_ref, b_ref):
    half = total // 4

    def get(t, r):
        one = main_ref[pl.ds(t * 8 + r, 8, stride=2), :]
        two = main_ref[pl.ds((t + half - 1) * 8 + r, 8, stride=2), :]
        return jnp.where(sublanes() < 4, one, two)

    out_ref[...] = tree(offs_ref, get, total, a_ref, b_ref)


def far_kernel(total, copies, offs_ref, main_ref, halo_ref, near_ref, out_ref, a_ref, b_ref):
    half = total // 4
    sub = sublanes()

    def get(t, r):
        head_one = main_ref[pl.ds(t * 8 + r + 4, 2, stride=2), :]
        head_two = main_ref[pl.ds((t + half) * 8 + r + 4, 2, stride=2), :]
        tail_one = halo_ref[pl.ds(t * 4 + r, 2, stride=2), :]
        tail_two = halo_ref[pl.ds((t + half) * 4 + r, 2, stride=2), :]
        return jnp.concatenate([head_one, tail_one, head_two, tail_two], axis=0)

    far = tree(offs_ref, get, total, a_ref, b_ref)
    both = jnp.where(sub % 4 < 2, near_ref[...], pltpu.roll(far, 2, axis=0))
    for k in range(copies // 2):
        out_ref[pl.ds(k * 8, 8), :] = both


def to_previous(count, groups):
    place = [q % count * groups + q // count for q in range(count * groups)]
    return list(zip(place[1:], place))


def local(spectrum, offsets):
    rows, span = spectrum.shape
    count = lax.axis_size("tm")
    groups = lax.axis_size("chan")
    total = rows * count
    cols = span // count // LANES
    tiles = spectrum.reshape(rows, span // LANES, LANES).transpose(1, 0, 2)
    main = lax.all_to_all(tiles, "tm", 0, 0, tiled=True)
    edge = main.reshape(count, cols, rows, LANES)[:, : cols // 2]
    halo = lax.ppermute(edge, ("tm", "chan"), to_previous(count, groups))
    main = main.reshape(-1, LANES)
    smem = pl.BlockSpec(memory_space=pltpu.SMEM)
    vmem = pl.BlockSpec(memory_space=pltpu.VMEM)
    scratch = [pltpu.VMEM((total // 2, 8, LANES), jnp.float32)] * 2
    params = pltpu.CompilerParams(vmem_limit_bytes=VMEM_LIMIT)
    cost = pl.CostEstimate(flops=20_000_000, bytes_accessed=600_000, transcendentals=0)
    near = pl.pallas_call(
        functools.partial(near_kernel, total),
        out_shape=jax.ShapeDtypeStruct((8, LANES), jnp.float32),
        in_specs=[smem, vmem],
        out_specs=vmem,
        scratch_shapes=scratch,
        compiler_params=params,
        cost_estimate=cost,
    )(offsets, main)
    best = pl.pallas_call(
        functools.partial(far_kernel, total, count),
        out_shape=jax.ShapeDtypeStruct((count * cols, LANES), jnp.float32),
        in_specs=[smem, vmem, vmem, vmem],
        out_specs=vmem,
        scratch_shapes=scratch,
        compiler_params=params,
        cost_estimate=cost,
    )(offsets, main, halo.reshape(-1, LANES), near)
    peak = lax.all_to_all(best, "tm", 0, 0, tiled=True)
    return peak.reshape(span)


def solution(mesh):
    placed = (P("tm", "chan"), P())
    return jax.shard_map(local, mesh=mesh, in_specs=placed, out_specs=P("chan"), check_vma=False)
```

```python
import functools

import jax
import jax.numpy as jnp
from jax import lax
from jax.experimental import pallas as pl
from jax.experimental.pallas import tpu as pltpu
from jax.sharding import PartitionSpec as P

LANES = 128
VMEM_LIMIT = 6 * 2**20


def sublanes():
    return lax.broadcasted_iota(jnp.int32, (8, LANES), 0)


def moved(upper, amount):
    lane = lax.broadcasted_iota(jnp.int32, (8, LANES), 1)
    turned = pltpu.roll(upper, (LANES - amount) & (LANES - 1), axis=1)
    return jnp.where(lane < LANES - amount, turned, pltpu.roll(turned, 7, axis=0))


def tree(offs_ref, get, total, a_ref, b_ref):
    half = total // 2
    for q in range(half // 2):
        lower, upper = get(q, 0), get(q, 1)
        for d in range(2):
            b_ref[2 * q + d] = lower + moved(upper, offs_ref[2 + d])
    src, dst = b_ref, a_ref
    length = 2
    while length < half:
        for p in range(length):
            amounts = [offs_ref[2 * length + 2 * p + odd] for odd in range(2)]
            for b in range(half // (2 * length)):
                lower = src[2 * b * length + p]
                upper = src[(2 * b + 1) * length + p]
                for odd in range(2):
                    dst[b * 2 * length + 2 * p + odd] = lower + moved(upper, amounts[odd])
        src, dst = dst, src
        length *= 2
    first = sublanes() < 4
    best = [jnp.full((8, LANES), -jnp.inf, jnp.float32) for _ in range(4)]
    for p in range(half):
        both = src[p]
        other = pltpu.roll(both, 4, axis=0)
        lower = jnp.where(first, both, other)
        even = moved(other, offs_ref[2 * length + 2 * p])
        odd = moved(both, offs_ref[2 * length + 2 * p + 1])
        best[p % 4] = jnp.maximum(best[p % 4], lower + jnp.where(first, even, odd))
    peak = functools.reduce(jnp.maximum, best)
    return jnp.maximum(peak, pltpu.roll(peak, 4, axis=0))


def near_kernel(total, spot, offs_ref, main_ref, out_ref, a_ref, b_ref):
    half = total // 4

    def get(t, r):
        one = main_ref[pl.ds(spot[t] * 8 + r, 4, stride=2), :]
        two = main_ref[pl.ds(spot[t + half] * 8 + r, 4, stride=2), :]
        return jnp.concatenate([one, two], axis=0)

    out_ref[...] = tree(offs_ref, get, total, a_ref, b_ref)


def far_kernel(total, copies, spot, offs_ref, more_ref, main_ref, halo_ref, near_ref, out_ref, a_ref, b_ref):
    half = total // 4
    sub = sublanes()
    keep = (sub % 4 < 2) | (more_ref[0] > 0)

    def get(t, r):
        one, two = spot[t], spot[t + half]
        head_one = main_ref[pl.ds(one * 8 + r + 4, 2, stride=2), :]
        head_two = main_ref[pl.ds(two * 8 + r + 4, 2, stride=2), :]
        tail_one = halo_ref[pl.ds(one * 4 + r, 2, stride=2), :]
        tail_two = halo_ref[pl.ds(two * 4 + r, 2, stride=2), :]
        both = jnp.concatenate([head_one, tail_one, head_two, tail_two], axis=0)
        return jnp.where(keep, both, 0.0)

    far = tree(offs_ref, get, total, a_ref, b_ref)
    both = jnp.where(sub % 4 < 2, near_ref[...], pltpu.roll(far, 2, axis=0))
    for k in range(copies // 2):
        out_ref[pl.ds(k * 8, 8), :] = both


def walk(count):
    side, cores = 4, 2
    plane = [(x, 0) for x in range(side)]
    for y in range(1, side):
        xs = range(1, side)
        plane += [(x, y) for x in (xs[::-1] if y % 2 else xs)]
    plane += [(0, y) for y in range(side - 1, 0, -1)]
    order = []
    for z in range(count // (side * side * cores)):
        for x, y in plane if z % 2 == 0 else plane[::-1]:
            order += [((z * side + x) * side + y) * cores + core for core in range(cores)]
    return order


def to_previous(order, groups):
    place = [t * groups + g for g in range(groups) for t in order]
    return list(zip(place, place[-1:] + place[:-1]))


def local(spectrum, offsets):
    rows, span = spectrum.shape
    count = lax.axis_size("tm")
    groups = lax.axis_size("chan")
    total = rows * count
    cols = span // count // LANES
    order = walk(count)
    spot = [order.index(t) for t in range(count)]
    more = (lax.axis_index("tm") != order[-1]) | (lax.axis_index("chan") != groups - 1)
    more = jnp.reshape(more, (1,)).astype(jnp.int32)
    tiles = spectrum.reshape(rows, span // LANES, LANES).transpose(1, 0, 2)
    main = lax.all_to_all(tiles, "tm", 0, 0, axis_index_groups=[order], tiled=True)
    edge = main.reshape(count, cols, rows, LANES)[:, : cols // 2]
    halo = lax.ppermute(edge, ("tm", "chan"), to_previous(order, groups))
    main = main.reshape(-1, LANES)
    smem = pl.BlockSpec(memory_space=pltpu.SMEM)
    vmem = pl.BlockSpec(memory_space=pltpu.VMEM)
    scratch = [pltpu.VMEM((total // 2, 8, LANES), jnp.float32)] * 2
    params = pltpu.CompilerParams(vmem_limit_bytes=VMEM_LIMIT)
    cost = pl.CostEstimate(flops=20_000_000, bytes_accessed=600_000, transcendentals=0)
    near = pl.pallas_call(
        functools.partial(near_kernel, total, spot),
        out_shape=jax.ShapeDtypeStruct((8, LANES), jnp.float32),
        in_specs=[smem, vmem],
        out_specs=vmem,
        scratch_shapes=scratch,
        compiler_params=params,
        cost_estimate=cost,
    )(offsets, main)
    best = pl.pallas_call(
        functools.partial(far_kernel, total, count, spot),
        out_shape=jax.ShapeDtypeStruct((count * cols, LANES), jnp.float32),
        in_specs=[smem, smem, vmem, vmem, vmem],
        out_specs=vmem,
        scratch_shapes=scratch,
        compiler_params=params,
        cost_estimate=cost,
    )(offsets, more, main, halo.reshape(-1, LANES), near)
    peak = lax.all_to_all(best, "tm", 0, 0, axis_index_groups=[order], tiled=True)
    return peak.reshape(span)


def solution(mesh):
    placed = (P("tm", "chan"), P())
    return jax.shard_map(local, mesh=mesh, in_specs=placed, out_specs=P("chan"), check_vma=False)
```

```python
import functools

import jax
import jax.numpy as jnp
from jax import lax
from jax.experimental import pallas as pl
from jax.experimental.pallas import tpu as pltpu
from jax.sharding import PartitionSpec as P

LANES = 128
VMEM_LIMIT = 6 * 2**20


def sublanes():
    return lax.broadcasted_iota(jnp.int32, (8, LANES), 0)


def moved(upper, amount):
    lane = lax.broadcasted_iota(jnp.int32, (8, LANES), 1)
    turned = pltpu.roll(upper, (LANES - amount) & (LANES - 1), axis=1)
    return jnp.where(lane < LANES - amount, turned, pltpu.roll(turned, 7, axis=0))


def tree(offs_ref, get, total, a_ref, b_ref):
    half = total // 2
    for q in range(half // 2):
        lower, upper = get(q, 0), get(q, 1)
        for d in range(2):
            b_ref[2 * q + d] = lower + moved(upper, offs_ref[2 + d])
    src, dst = b_ref, a_ref
    length = 2
    while length < half:
        for p in range(length):
            amounts = [offs_ref[2 * length + 2 * p + odd] for odd in range(2)]
            for b in range(half // (2 * length)):
                lower = src[2 * b * length + p]
                upper = src[(2 * b + 1) * length + p]
                for odd in range(2):
                    dst[b * 2 * length + 2 * p + odd] = lower + moved(upper, amounts[odd])
        src, dst = dst, src
        length *= 2
    first = sublanes() < 4
    best = [jnp.full((8, LANES), -jnp.inf, jnp.float32) for _ in range(4)]
    for p in range(half):
        both = src[p]
        other = pltpu.roll(both, 4, axis=0)
        lower = jnp.where(first, both, other)
        even = moved(other, offs_ref[2 * length + 2 * p])
        odd = moved(both, offs_ref[2 * length + 2 * p + 1])
        best[p % 4] = jnp.maximum(best[p % 4], lower + jnp.where(first, even, odd))
    peak = functools.reduce(jnp.maximum, best)
    return jnp.maximum(peak, pltpu.roll(peak, 4, axis=0))


def near_kernel(total, spot, offs_ref, main_ref, out_ref, a_ref, b_ref):
    half = total // 4

    def get(t, r):
        one = main_ref[pl.ds(spot[t] * 8 + r, 4, stride=2), :]
        two = main_ref[pl.ds(spot[t + half] * 8 + r, 4, stride=2), :]
        return jnp.concatenate([one, two], axis=0)

    out_ref[...] = tree(offs_ref, get, total, a_ref, b_ref)


def far_kernel(total, copies, spot, offs_ref, more_ref, main_ref, halo_ref, near_ref, out_ref, a_ref, b_ref):
    half = total // 4
    sub = sublanes()
    keep = (sub % 4 < 2) | (more_ref[0] > 0)

    def get(t, r):
        one, two = spot[t], spot[t + half]
        head_one = main_ref[pl.ds(one * 8 + r + 4, 2, stride=2), :]
        head_two = main_ref[pl.ds(two * 8 + r + 4, 2, stride=2), :]
        tail_one = halo_ref[pl.ds(one * 4 + r, 2, stride=2), :]
        tail_two = halo_ref[pl.ds(two * 4 + r, 2, stride=2), :]
        both = jnp.concatenate([head_one, tail_one, head_two, tail_two], axis=0)
        return jnp.where(keep, both, 0.0)

    far = tree(offs_ref, get, total, a_ref, b_ref)
    both = jnp.where(sub % 4 < 2, near_ref[...], pltpu.roll(far, 2, axis=0))
    for k in range(copies // 2):
        out_ref[pl.ds(k * 8, 8), :] = both


def walk(count):
    side, cores = 4, 2
    plane = [(x, 0) for x in range(side)]
    for y in range(1, side):
        xs = range(1, side)
        plane += [(x, y) for x in (xs[::-1] if y % 2 else xs)]
    plane += [(0, y) for y in range(side - 1, 0, -1)]
    order = []
    for z in range(count // (side * side * cores)):
        for x, y in plane if z % 2 == 0 else plane[::-1]:
            order += [((z * side + x) * side + y) * cores + core for core in range(cores)]
    return order


def to_previous(order, groups):
    place = [t * groups + g for g in range(groups) for t in order]
    return list(zip(place, place[-1:] + place[:-1]))


def local(spectrum, offsets):
    rows, span = spectrum.shape
    count = lax.axis_size("tm")
    groups = lax.axis_size("chan")
    total = rows * count
    cols = span // count // LANES
    order = walk(count)
    spot = [order.index(t) for t in range(count)]
    more = (lax.axis_index("tm") != order[-1]) | (lax.axis_index("chan") != groups - 1)
    more = jnp.reshape(more, (1,)).astype(jnp.int32)
    tiles = spectrum.reshape(rows, span // LANES, LANES).transpose(1, 0, 2)
    main = lax.all_to_all(tiles, "tm", 0, 0, axis_index_groups=[order], tiled=True)
    edge = main.reshape(count, cols, rows, LANES)[:, : cols // 2]
    halo = lax.ppermute(edge, ("tm", "chan"), to_previous(order, groups))
    main = main.reshape(-1, LANES)
    smem = pl.BlockSpec(memory_space=pltpu.SMEM)
    vmem = pl.BlockSpec(memory_space=pltpu.VMEM)
    scratch = [pltpu.VMEM((total // 2, 8, LANES), jnp.float32)] * 2
    params = pltpu.CompilerParams(vmem_limit_bytes=VMEM_LIMIT)
    cost = pl.CostEstimate(flops=20_000_000, bytes_accessed=600_000, transcendentals=0)
    near = pl.pallas_call(
        functools.partial(near_kernel, total, spot),
        out_shape=jax.ShapeDtypeStruct((8, LANES), jnp.float32),
        in_specs=[smem, vmem],
        out_specs=vmem,
        scratch_shapes=scratch,
        compiler_params=params,
        cost_estimate=cost,
    )(offsets, main)
    best = pl.pallas_call(
        functools.partial(far_kernel, total, count // 2, spot),
        out_shape=jax.ShapeDtypeStruct((count // 2 * cols, LANES), jnp.float32),
        in_specs=[smem, smem, vmem, vmem, vmem],
        out_specs=vmem,
        scratch_shapes=scratch,
        compiler_params=params,
        cost_estimate=cost,
    )(offsets, more, main, halo.reshape(-1, LANES), near)
    cores = [order[core::2] for core in range(2)]
    ours = lax.all_to_all(best, "tm", 0, 0, axis_index_groups=cores, tiled=True)
    theirs = lax.ppermute(ours, "tm", [(t, t ^ 1) for t in range(count)])
    pair = [part.reshape(count // 2, 1, cols, LANES) for part in (ours, theirs)]
    second = lax.axis_index("tm") % 2 == 1
    first_core = jnp.where(second, pair[1], pair[0])
    second_core = jnp.where(second, pair[0], pair[1])
    return jnp.concatenate([first_core, second_core], axis=1).reshape(span)


def solution(mesh):
    placed = (P("tm", "chan"), P())
    return jax.shard_map(local, mesh=mesh, in_specs=placed, out_specs=P("chan"), check_vma=False)
```

```python
import functools

import jax
import jax.numpy as jnp
from jax import lax
from jax.experimental import pallas as pl
from jax.experimental.pallas import tpu as pltpu
from jax.sharding import PartitionSpec as P

LANES = 128
VMEM_LIMIT = 6 * 2**20
CHIPS = (
    6, 10, 14, 13, 12, 8, 9, 5, 21, 22, 23, 7, 3, 2, 1, 0,
    4, 20, 16, 32, 36, 52, 48, 49, 53, 57, 58, 59, 43, 39, 38, 42,
    46, 45, 44, 28, 24, 40, 56, 60, 61, 62, 63, 47, 31, 15, 11, 27,
    26, 30, 29, 25, 41, 37, 33, 17, 18, 19, 35, 34, 50, 51, 55, 54,
)


def sublanes():
    return lax.broadcasted_iota(jnp.int32, (8, LANES), 0)


def moved(upper, amount):
    lane = lax.broadcasted_iota(jnp.int32, (8, LANES), 1)
    turned = pltpu.roll(upper, (LANES - amount) & (LANES - 1), axis=1)
    return jnp.where(lane < LANES - amount, turned, pltpu.roll(turned, 7, axis=0))


def tree(offs_ref, get, total, a_ref, b_ref):
    half = total // 2
    for q in range(half // 2):
        lower, upper = get(q, 0), get(q, 1)
        for d in range(2):
            b_ref[2 * q + d] = lower + moved(upper, offs_ref[2 + d])
    src, dst = b_ref, a_ref
    length = 2
    while length < half:
        for p in range(length):
            amounts = [offs_ref[2 * length + 2 * p + odd] for odd in range(2)]
            for b in range(half // (2 * length)):
                lower = src[2 * b * length + p]
                upper = src[(2 * b + 1) * length + p]
                for odd in range(2):
                    dst[b * 2 * length + 2 * p + odd] = lower + moved(upper, amounts[odd])
        src, dst = dst, src
        length *= 2
    first = sublanes() < 4
    best = [jnp.full((8, LANES), -jnp.inf, jnp.float32) for _ in range(4)]
    for p in range(half):
        both = src[p]
        other = pltpu.roll(both, 4, axis=0)
        lower = jnp.where(first, both, other)
        even = moved(other, offs_ref[2 * length + 2 * p])
        odd = moved(both, offs_ref[2 * length + 2 * p + 1])
        best[p % 4] = jnp.maximum(best[p % 4], lower + jnp.where(first, even, odd))
    peak = functools.reduce(jnp.maximum, best)
    return jnp.maximum(peak, pltpu.roll(peak, 4, axis=0))


def near_kernel(total, spot, table_ref, main_ref, out_ref, offs_ref, a_ref, b_ref, sem):
    half = total // 4
    copy = pltpu.make_async_copy(table_ref, offs_ref, sem)
    copy.start()
    copy.wait()

    def get(t, r):
        one = main_ref[pl.ds(spot[t] * 8 + r, 4, stride=2), :]
        two = main_ref[pl.ds(spot[t + half] * 8 + r, 4, stride=2), :]
        return jnp.concatenate([one, two], axis=0)

    out_ref[...] = tree(offs_ref, get, total, a_ref, b_ref)


def far_kernel(total, copies, spot, offs_ref, more_ref, main_ref, halo_ref, near_ref, out_ref, a_ref, b_ref):
    half = total // 4
    sub = sublanes()
    keep = (sub % 4 < 2) | (more_ref[0] > 0)

    def get(t, r):
        one, two = spot[t], spot[t + half]
        head_one = main_ref[pl.ds(one * 8 + r + 4, 2, stride=2), :]
        head_two = main_ref[pl.ds(two * 8 + r + 4, 2, stride=2), :]
        tail_one = halo_ref[pl.ds(one * 4 + r, 2, stride=2), :]
        tail_two = halo_ref[pl.ds(two * 4 + r, 2, stride=2), :]
        both = jnp.concatenate([head_one, tail_one, head_two, tail_two], axis=0)
        return jnp.where(keep, both, 0.0)

    far = tree(offs_ref, get, total, a_ref, b_ref)
    both = jnp.where(sub % 4 < 2, near_ref[...], pltpu.roll(far, 2, axis=0))
    for k in range(copies // 2):
        out_ref[pl.ds(k * 8, 8), :] = both


def walk(count):
    assert count == 2 * len(CHIPS)
    return [2 * chip + core for chip in CHIPS for core in range(2)]


def to_previous(order, groups):
    place = [t * groups + g for g in range(groups) for t in order]
    return list(zip(place, place[-1:] + place[:-1]))


def local(spectrum, offsets):
    rows, span = spectrum.shape
    count = lax.axis_size("tm")
    groups = lax.axis_size("chan")
    total = rows * count
    cols = span // count // LANES
    order = walk(count)
    spot = [order.index(t) for t in range(count)]
    more = (lax.axis_index("tm") != order[-1]) | (lax.axis_index("chan") != groups - 1)
    more = jnp.reshape(more, (1,)).astype(jnp.int32)
    tiles = spectrum.reshape(rows, span // LANES, LANES).transpose(1, 0, 2)
    main = lax.all_to_all(tiles, "tm", 0, 0, axis_index_groups=[order], tiled=True)
    edge = main.reshape(count, cols, rows, LANES)[:, : cols // 2]
    halo = lax.ppermute(edge, ("tm", "chan"), to_previous(order, groups))
    main = main.reshape(-1, LANES)
    smem = pl.BlockSpec(memory_space=pltpu.SMEM)
    vmem = pl.BlockSpec(memory_space=pltpu.VMEM)
    scratch = [pltpu.VMEM((total // 2, 8, LANES), jnp.float32)] * 2
    params = pltpu.CompilerParams(vmem_limit_bytes=VMEM_LIMIT)
    cost = pl.CostEstimate(flops=20_000_000, bytes_accessed=600_000, transcendentals=0)
    near, table = pl.pallas_call(
        functools.partial(near_kernel, total, spot),
        out_shape=(jax.ShapeDtypeStruct((8, LANES), jnp.float32), pltpu.SMEM(offsets.shape, jnp.int32)),
        in_specs=[pl.BlockSpec(memory_space=pl.ANY), vmem],
        out_specs=(vmem, smem),
        scratch_shapes=scratch + [pltpu.SemaphoreType.DMA],
        compiler_params=params,
        cost_estimate=cost,
    )(offsets, main)
    best = pl.pallas_call(
        functools.partial(far_kernel, total, count // 2, spot),
        out_shape=jax.ShapeDtypeStruct((count // 2 * cols, LANES), jnp.float32),
        in_specs=[smem, smem, vmem, vmem, vmem],
        out_specs=vmem,
        scratch_shapes=scratch,
        compiler_params=params,
        cost_estimate=cost,
    )(table, more, main, halo.reshape(-1, LANES), near)
    cores = [order[core::2] for core in range(2)]
    ours = lax.all_to_all(best, "tm", 0, 0, axis_index_groups=cores, tiled=True)
    theirs = lax.ppermute(ours, "tm", [(t, t ^ 1) for t in range(count)])
    pair = [part.reshape(count // 2, 1, cols, LANES) for part in (ours, theirs)]
    second = lax.axis_index("tm") % 2 == 1
    first_core = jnp.where(second, pair[1], pair[0])
    second_core = jnp.where(second, pair[0], pair[1])
    return jnp.concatenate([first_core, second_core], axis=1).reshape(span)


def solution(mesh):
    placed = (P("tm", "chan"), P())
    return jax.shard_map(local, mesh=mesh, in_specs=placed, out_specs=P("chan"), check_vma=False)
```

```python
import functools

import jax
import jax.numpy as jnp
from jax import lax
from jax.experimental import pallas as pl
from jax.experimental.pallas import tpu as pltpu
from jax.sharding import PartitionSpec as P

LANES = 128
VMEM_LIMIT = 6 * 2**20
CHIPS = (
    10, 26, 25, 24, 28, 12, 8, 4, 0, 16, 20, 21, 22, 23, 27, 31,
    30, 14, 15, 11, 7, 3, 19, 18, 17, 1, 2, 6, 5, 9, 13, 29,
    45, 46, 47, 63, 59, 55, 51, 50, 54, 53, 57, 56, 52, 48, 49, 33,
    32, 36, 37, 38, 34, 35, 39, 43, 42, 41, 40, 44, 60, 61, 62, 58,
)


def sublanes():
    return lax.broadcasted_iota(jnp.int32, (8, LANES), 0)


def moved(upper, amount):
    lane = lax.broadcasted_iota(jnp.int32, (8, LANES), 1)
    turned = pltpu.roll(upper, (LANES - amount) & (LANES - 1), axis=1)
    return jnp.where(lane < LANES - amount, turned, pltpu.roll(turned, 7, axis=0))


def tree(offs_ref, get, total, a_ref, b_ref):
    half = total // 2
    step = jnp.full((8, LANES), offs_ref[2], jnp.int32) > 0
    for q in range(half // 2):
        lower, upper = get(q, 0), get(q, 1)
        by_one = moved(upper, 1)
        b_ref[2 * q] = lower + jnp.where(step, by_one, upper)
        b_ref[2 * q + 1] = lower + by_one
    src, dst = b_ref, a_ref
    length = 2
    while length < half:
        for p in range(length):
            amounts = [offs_ref[2 * length + 2 * p + odd] for odd in range(2)]
            for b in range(half // (2 * length)):
                lower = src[2 * b * length + p]
                upper = src[(2 * b + 1) * length + p]
                for odd in range(2):
                    dst[b * 2 * length + 2 * p + odd] = lower + moved(upper, amounts[odd])
        src, dst = dst, src
        length *= 2
    first = sublanes() < 4
    best = [jnp.full((8, LANES), -jnp.inf, jnp.float32) for _ in range(4)]
    for p in range(half):
        both = src[p]
        other = pltpu.roll(both, 4, axis=0)
        lower = jnp.where(first, both, other)
        even = moved(other, offs_ref[2 * length + 2 * p])
        odd = moved(both, offs_ref[2 * length + 2 * p + 1])
        best[p % 4] = jnp.maximum(best[p % 4], lower + jnp.where(first, even, odd))
    peak = functools.reduce(jnp.maximum, best)
    return jnp.maximum(peak, pltpu.roll(peak, 4, axis=0))


def near_kernel(total, spot, table_ref, main_ref, out_ref, offs_ref, a_ref, b_ref, sem):
    half = total // 4
    copy = pltpu.make_async_copy(table_ref, offs_ref, sem)
    copy.start()
    copy.wait()

    def get(t, r):
        one = main_ref[pl.ds(spot[t] * 8 + r, 4, stride=2), :]
        two = main_ref[pl.ds(spot[t + half] * 8 + r, 4, stride=2), :]
        return jnp.concatenate([one, two], axis=0)

    out_ref[...] = tree(offs_ref, get, total, a_ref, b_ref)


def far_kernel(total, copies, spot, offs_ref, more_ref, main_ref, halo_ref, near_ref, out_ref, a_ref, b_ref):
    half = total // 4
    sub = sublanes()
    keep = (sub % 4 < 2) | (more_ref[0] > 0)

    def get(t, r):
        one, two = spot[t], spot[t + half]
        head_one = main_ref[pl.ds(one * 8 + r + 4, 2, stride=2), :]
        head_two = main_ref[pl.ds(two * 8 + r + 4, 2, stride=2), :]
        tail_one = halo_ref[pl.ds(3 * half * r + one, 2, stride=half), :]
        tail_two = halo_ref[pl.ds(3 * half * r + two, 2, stride=half), :]
        both = jnp.concatenate([head_one, tail_one, head_two, tail_two], axis=0)
        return jnp.where(keep, both, 0.0)

    far = tree(offs_ref, get, total, a_ref, b_ref)
    both = jnp.where(sub % 4 < 2, near_ref[...], pltpu.roll(far, 2, axis=0))
    for k in range(copies // 2):
        out_ref[pl.ds(k * 8, 8), :] = both


def walk(count):
    assert count == 2 * len(CHIPS)
    return [2 * chip + core for chip in CHIPS for core in range(2)]


def to_previous(order, groups):
    place = [t * groups + g for g in range(groups) for t in order]
    return list(zip(place, place[-1:] + place[:-1]))


def local(spectrum, offsets):
    rows, span = spectrum.shape
    count = lax.axis_size("tm")
    groups = lax.axis_size("chan")
    total = rows * count
    cols = span // count // LANES
    order = walk(count)
    spot = [order.index(t) for t in range(count)]
    more = (lax.axis_index("tm") != order[-1]) | (lax.axis_index("chan") != groups - 1)
    more = jnp.reshape(more, (1,)).astype(jnp.int32)
    tiles = spectrum.reshape(rows, span // LANES, LANES).transpose(1, 0, 2)
    main = lax.all_to_all(tiles, "tm", 0, 0, axis_index_groups=[order], tiled=True)
    early = count // 2
    assert max(order[:early]) < early
    window = main.reshape(count, cols, rows, LANES)
    edge = jnp.concatenate([window[:, 0], window[early:, 1]], axis=0)
    halo = lax.ppermute(edge, ("tm", "chan"), to_previous(order, groups))
    main = main.reshape(-1, LANES)
    smem = pl.BlockSpec(memory_space=pltpu.SMEM)
    vmem = pl.BlockSpec(memory_space=pltpu.VMEM)
    scratch = [pltpu.VMEM((total // 2, 8, LANES), jnp.float32)] * 2
    params = pltpu.CompilerParams(vmem_limit_bytes=VMEM_LIMIT)
    cost = pl.CostEstimate(flops=20_000_000, bytes_accessed=600_000, transcendentals=0)
    near, table = pl.pallas_call(
        functools.partial(near_kernel, total, spot),
        out_shape=(jax.ShapeDtypeStruct((8, LANES), jnp.float32), pltpu.SMEM(offsets.shape, jnp.int32)),
        in_specs=[pl.BlockSpec(memory_space=pl.ANY), vmem],
        out_specs=(vmem, smem),
        scratch_shapes=scratch + [pltpu.SemaphoreType.DMA],
        compiler_params=params,
        cost_estimate=cost,
    )(offsets, main)
    best = pl.pallas_call(
        functools.partial(far_kernel, total, count // 2, spot),
        out_shape=jax.ShapeDtypeStruct((count // 2 * cols, LANES), jnp.float32),
        in_specs=[smem, smem, vmem, vmem, vmem],
        out_specs=vmem,
        scratch_shapes=scratch,
        compiler_params=params,
        cost_estimate=cost,
    )(table, more, main, halo.transpose(1, 0, 2).reshape(-1, LANES), near)
    cores = [order[core::2] for core in range(2)]
    ours = lax.all_to_all(best, "tm", 0, 0, axis_index_groups=cores, tiled=True)
    theirs = lax.ppermute(ours, "tm", [(t, t ^ 1) for t in range(count)])
    pair = [part.reshape(count // 2, 1, cols, LANES) for part in (ours, theirs)]
    second = lax.axis_index("tm") % 2 == 1
    first_core = jnp.where(second, pair[1], pair[0])
    second_core = jnp.where(second, pair[0], pair[1])
    return jnp.concatenate([first_core, second_core], axis=1).reshape(span)


def solution(mesh):
    placed = (P("tm", "chan"), P())
    return jax.shard_map(local, mesh=mesh, in_specs=placed, out_specs=P("chan"), check_vma=False)
```

```python
import functools

import jax
import jax.numpy as jnp
from jax import lax
from jax.experimental import pallas as pl
from jax.experimental.pallas import tpu as pltpu
from jax.sharding import PartitionSpec as P

LANES = 128
VMEM_LIMIT = 6 * 2**20
CHIPS = (
    10, 14, 15, 31, 27, 11, 7, 6, 5, 9, 13, 12, 28, 29, 30, 26,
    25, 24, 8, 4, 20, 16, 0, 1, 2, 3, 19, 23, 22, 18, 17, 21,
    37, 38, 39, 35, 51, 55, 59, 43, 42, 41, 57, 61, 62, 63, 47, 46,
    45, 44, 60, 56, 40, 36, 32, 48, 52, 53, 49, 33, 34, 50, 54, 58,
)


def sublanes():
    return lax.broadcasted_iota(jnp.int32, (8, LANES), 0)


def moved(upper, amount):
    lane = lax.broadcasted_iota(jnp.int32, (8, LANES), 1)
    turned = pltpu.roll(upper, (LANES - amount) & (LANES - 1), axis=1)
    return jnp.where(lane < LANES - amount, turned, pltpu.roll(turned, 7, axis=0))


def tree(offs_ref, get, total, a_ref, b_ref):
    half = total // 2
    step = jnp.full((8, LANES), offs_ref[2], jnp.int32) > 0
    for q in range(half // 2):
        lower, upper = get(q, 0), get(q, 1)
        by_one = moved(upper, 1)
        b_ref[2 * q] = lower + jnp.where(step, by_one, upper)
        b_ref[2 * q + 1] = lower + by_one
    src, dst = b_ref, a_ref
    length = 2
    while length < half:
        for p in range(length):
            amounts = [offs_ref[2 * length + 2 * p + odd] for odd in range(2)]
            for b in range(half // (2 * length)):
                lower = src[2 * b * length + p]
                upper = src[(2 * b + 1) * length + p]
                for odd in range(2):
                    dst[b * 2 * length + 2 * p + odd] = lower + moved(upper, amounts[odd])
        src, dst = dst, src
        length *= 2
    first = sublanes() < 4
    best = [jnp.full((8, LANES), -jnp.inf, jnp.float32) for _ in range(4)]
    for p in range(half):
        both = src[p]
        other = pltpu.roll(both, 4, axis=0)
        lower = jnp.where(first, both, other)
        even = moved(other, offs_ref[2 * length + 2 * p])
        odd = moved(both, offs_ref[2 * length + 2 * p + 1])
        best[p % 4] = jnp.maximum(best[p % 4], lower + jnp.where(first, even, odd))
    peak = functools.reduce(jnp.maximum, best)
    return jnp.maximum(peak, pltpu.roll(peak, 4, axis=0))


def near_kernel(total, spot, table_ref, main_ref, out_ref, offs_ref, a_ref, b_ref, sem):
    half = total // 4
    copy = pltpu.make_async_copy(table_ref, offs_ref, sem)
    copy.start()
    copy.wait()

    def get(t, r):
        one = main_ref[pl.ds(spot[t] * 8 + r, 4, stride=2), :]
        two = main_ref[pl.ds(spot[t + half] * 8 + r, 4, stride=2), :]
        return jnp.concatenate([one, two], axis=0)

    out_ref[...] = tree(offs_ref, get, total, a_ref, b_ref)


def far_kernel(total, copies, spot, offs_ref, more_ref, main_ref, halo_ref, near_ref, out_ref, a_ref, b_ref):
    half = total // 4
    sub = sublanes()
    keep = (sub % 4 < 2) | (more_ref[0] > 0)

    def get(t, r):
        one, two = spot[t], spot[t + half]
        head_one = main_ref[pl.ds(one * 8 + r + 4, 2, stride=2), :]
        head_two = main_ref[pl.ds(two * 8 + r + 4, 2, stride=2), :]
        tail_one = halo_ref[pl.ds(3 * half * r + one, 2, stride=half), :]
        tail_two = halo_ref[pl.ds(3 * half * r + two, 2, stride=half), :]
        both = jnp.concatenate([head_one, tail_one, head_two, tail_two], axis=0)
        return jnp.where(keep, both, 0.0)

    far = tree(offs_ref, get, total, a_ref, b_ref)
    both = jnp.where(sub % 4 < 2, near_ref[...], pltpu.roll(far, 2, axis=0))
    for k in range(copies // 2):
        out_ref[pl.ds(k * 8, 8), :] = both


def walk(count):
    assert count == 2 * len(CHIPS)
    return [2 * chip + core for chip in CHIPS for core in range(2)]


def to_previous(order, groups):
    place = [t * groups + g for g in range(groups) for t in order]
    return list(zip(place, place[-1:] + place[:-1]))


def local(spectrum, offsets):
    rows, span = spectrum.shape
    count = lax.axis_size("tm")
    groups = lax.axis_size("chan")
    total = rows * count
    cols = span // count // LANES
    order = walk(count)
    spot = [order.index(t) for t in range(count)]
    more = (lax.axis_index("tm") != order[-1]) | (lax.axis_index("chan") != groups - 1)
    more = jnp.reshape(more, (1,)).astype(jnp.int32)
    tiles = spectrum.reshape(rows, span // LANES, LANES).transpose(1, 0, 2)
    main = lax.all_to_all(tiles, "tm", 0, 0, axis_index_groups=[order], tiled=True)
    early = count // 2
    assert max(order[:early]) < early
    window = main.reshape(count, cols, rows, LANES)
    edge = jnp.concatenate([window[:, 0], window[early:, 1]], axis=0)
    halo = lax.ppermute(edge, ("tm", "chan"), to_previous(order, groups))
    main = main.reshape(-1, LANES)
    smem = pl.BlockSpec(memory_space=pltpu.SMEM)
    vmem = pl.BlockSpec(memory_space=pltpu.VMEM)
    scratch = [pltpu.VMEM((total // 2, 8, LANES), jnp.float32)] * 2
    params = pltpu.CompilerParams(vmem_limit_bytes=VMEM_LIMIT)
    cost = pl.CostEstimate(flops=20_000_000, bytes_accessed=600_000, transcendentals=0)
    near, table = pl.pallas_call(
        functools.partial(near_kernel, total, spot),
        out_shape=(jax.ShapeDtypeStruct((8, LANES), jnp.float32), pltpu.SMEM(offsets.shape, jnp.int32)),
        in_specs=[pl.BlockSpec(memory_space=pl.ANY), vmem],
        out_specs=(vmem, smem),
        scratch_shapes=scratch + [pltpu.SemaphoreType.DMA],
        compiler_params=params,
        cost_estimate=cost,
    )(offsets, main)
    best = pl.pallas_call(
        functools.partial(far_kernel, total, count // 2, spot),
        out_shape=jax.ShapeDtypeStruct((count // 2 * cols, LANES), jnp.float32),
        in_specs=[smem, smem, vmem, vmem, vmem],
        out_specs=vmem,
        scratch_shapes=scratch,
        compiler_params=params,
        cost_estimate=cost,
    )(table, more, main, halo.transpose(1, 0, 2).reshape(-1, LANES), near)
    cores = [order[core::2] for core in range(2)]
    ours = lax.all_to_all(best, "tm", 0, 0, axis_index_groups=cores, tiled=True)
    theirs = lax.ppermute(ours, "tm", [(t, t ^ 1) for t in range(count)])
    pair = [part.reshape(count // 2, 1, cols, LANES) for part in (ours, theirs)]
    second = lax.axis_index("tm") % 2 == 1
    first_core = jnp.where(second, pair[1], pair[0])
    second_core = jnp.where(second, pair[0], pair[1])
    return jnp.concatenate([first_core, second_core], axis=1).reshape(span)


def solution(mesh):
    placed = (P("tm", "chan"), P())
    return jax.shard_map(local, mesh=mesh, in_specs=placed, out_specs=P("chan"), check_vma=False)
```

```python
import functools

import jax
import jax.numpy as jnp
from jax import lax
from jax.experimental import pallas as pl
from jax.experimental.pallas import tpu as pltpu
from jax.sharding import PartitionSpec as P

LANES = 128
VMEM_LIMIT = 6 * 2**20
CHIPS = (
    10, 14, 15, 31, 27, 11, 7, 6, 5, 9, 13, 12, 28, 29, 30, 26,
    25, 24, 8, 4, 20, 16, 0, 1, 2, 3, 19, 23, 22, 18, 17, 21,
    37, 38, 39, 35, 51, 55, 59, 43, 42, 41, 57, 61, 62, 63, 47, 46,
    45, 44, 60, 56, 40, 36, 32, 48, 52, 53, 49, 33, 34, 50, 54, 58,
)
LEAD = 40


def sublanes():
    return lax.broadcasted_iota(jnp.int32, (8, LANES), 0)


def moved(upper, amount):
    lane = lax.broadcasted_iota(jnp.int32, (8, LANES), 1)
    turned = pltpu.roll(upper, (LANES - amount) & (LANES - 1), axis=1)
    return jnp.where(lane < LANES - amount, turned, pltpu.roll(turned, 7, axis=0))


def tree(offs_ref, get, total, a_ref, b_ref):
    half = total // 2
    step = jnp.full((8, LANES), offs_ref[2], jnp.int32) > 0
    for q in range(half // 2):
        lower, upper = get(q, 0), get(q, 1)
        by_one = moved(upper, 1)
        b_ref[2 * q] = lower + jnp.where(step, by_one, upper)
        b_ref[2 * q + 1] = lower + by_one
    src, dst = b_ref, a_ref
    length = 2
    while length < half:
        for p in range(length):
            amounts = [offs_ref[2 * length + 2 * p + odd] for odd in range(2)]
            for b in range(half // (2 * length)):
                lower = src[2 * b * length + p]
                upper = src[(2 * b + 1) * length + p]
                for odd in range(2):
                    dst[b * 2 * length + 2 * p + odd] = lower + moved(upper, amounts[odd])
        src, dst = dst, src
        length *= 2
    first = sublanes() < 4
    best = [jnp.full((8, LANES), -jnp.inf, jnp.float32) for _ in range(4)]
    for p in range(half):
        both = src[p]
        other = pltpu.roll(both, 4, axis=0)
        lower = jnp.where(first, both, other)
        even = moved(other, offs_ref[2 * length + 2 * p])
        odd = moved(both, offs_ref[2 * length + 2 * p + 1])
        best[p % 4] = jnp.maximum(best[p % 4], lower + jnp.where(first, even, odd))
    peak = functools.reduce(jnp.maximum, best)
    return jnp.maximum(peak, pltpu.roll(peak, 4, axis=0))


def near_kernel(total, spot, table_ref, main_ref, out_ref, offs_ref, a_ref, b_ref, sem):
    half = total // 4
    copy = pltpu.make_async_copy(table_ref, offs_ref, sem)
    copy.start()
    copy.wait()

    def get(t, r):
        one = main_ref[pl.ds(spot[t] * 8 + r, 4, stride=2), :]
        two = main_ref[pl.ds(spot[t + half] * 8 + r, 4, stride=2), :]
        return jnp.concatenate([one, two], axis=0)

    out_ref[...] = tree(offs_ref, get, total, a_ref, b_ref)


def far_kernel(total, copies, spot, offs_ref, more_ref, main_ref, halo_ref, near_ref, out_ref, a_ref, b_ref):
    half = total // 4
    sub = sublanes()
    keep = (sub % 4 < 2) | (more_ref[0] > 0)

    def get(t, r):
        one, two = spot[t], spot[t + half]
        head_one = main_ref[pl.ds(one * 8 + r + 4, 2, stride=2), :]
        head_two = main_ref[pl.ds(two * 8 + r + 4, 2, stride=2), :]
        tail_one = halo_ref[pl.ds(3 * half * r + one, 2, stride=half), :]
        tail_two = halo_ref[pl.ds(3 * half * r + two, 2, stride=half), :]
        both = jnp.concatenate([head_one, tail_one, head_two, tail_two], axis=0)
        return jnp.where(keep, both, 0.0)

    far = tree(offs_ref, get, total, a_ref, b_ref)
    both = jnp.where(sub % 4 < 2, near_ref[...], pltpu.roll(far, 2, axis=0))
    for k in range(copies // 2):
        out_ref[pl.ds(k * 8, 8), :] = both


def walk(count):
    assert count == 2 * len(CHIPS)
    return [2 * chip + core for chip in CHIPS for core in range(2)]


def to_previous(order, groups):
    place = [t * groups + g for g in range(groups) for t in order]
    return list(zip(place, place[-1:] + place[:-1]))


def local(spectrum, offsets):
    rows, span = spectrum.shape
    count = lax.axis_size("tm")
    groups = lax.axis_size("chan")
    total = rows * count
    cols = span // count // LANES
    order = walk(count)
    spot = [order.index(t) for t in range(count)]
    more = (lax.axis_index("tm") != order[-1]) | (lax.axis_index("chan") != groups - 1)
    more = jnp.reshape(more, (1,)).astype(jnp.int32)
    tiles = spectrum.reshape(rows, span // LANES, LANES).transpose(1, 0, 2)
    main = lax.all_to_all(tiles, "tm", 0, 0, axis_index_groups=[order], tiled=True)
    early = count // 2
    assert max(order[:early]) < early
    window = main.reshape(count, cols, rows, LANES)
    edge = jnp.concatenate([window[:, 0], window[early:, 1]], axis=0)
    halo = lax.ppermute(edge, ("tm", "chan"), to_previous(order, groups))
    main = main.reshape(-1, LANES)
    smem = pl.BlockSpec(memory_space=pltpu.SMEM)
    vmem = pl.BlockSpec(memory_space=pltpu.VMEM)
    scratch = [pltpu.VMEM((total // 2, 8, LANES), jnp.float32)] * 2
    params = pltpu.CompilerParams(vmem_limit_bytes=VMEM_LIMIT)
    cost = pl.CostEstimate(flops=20_000_000, bytes_accessed=600_000, transcendentals=0)
    near, table = pl.pallas_call(
        functools.partial(near_kernel, total, spot),
        out_shape=(jax.ShapeDtypeStruct((8, LANES), jnp.float32), pltpu.SMEM(offsets.shape, jnp.int32)),
        in_specs=[pl.BlockSpec(memory_space=pl.ANY), vmem],
        out_specs=(vmem, smem),
        scratch_shapes=scratch + [pltpu.SemaphoreType.DMA],
        compiler_params=params,
        cost_estimate=cost,
    )(offsets, main)
    best = pl.pallas_call(
        functools.partial(far_kernel, total, count // 2, spot),
        out_shape=jax.ShapeDtypeStruct((count // 2 * cols, LANES), jnp.float32),
        in_specs=[smem, smem, vmem, vmem, vmem],
        out_specs=vmem,
        scratch_shapes=scratch,
        compiler_params=params,
        cost_estimate=cost,
    )(table, more, main, halo.transpose(1, 0, 2).reshape(-1, LANES), near)
    turned = order[2 * LEAD :] + order[: 2 * LEAD]
    cores = [turned[core::2] for core in range(2)]
    ours = lax.all_to_all(best, "tm", 0, 0, axis_index_groups=cores, tiled=True)
    theirs = lax.ppermute(ours, "tm", [(t, t ^ 1) for t in range(count)])
    pair = [part.reshape(count // 2, 1, cols, LANES) for part in (ours, theirs)]
    second = lax.axis_index("tm") % 2 == 1
    first_core = jnp.where(second, pair[1], pair[0])
    second_core = jnp.where(second, pair[0], pair[1])
    both = jnp.concatenate([first_core, second_core], axis=1)
    return jnp.roll(both, LEAD, axis=0).reshape(span)


def solution(mesh):
    placed = (P("tm", "chan"), P())
    return jax.shard_map(local, mesh=mesh, in_specs=placed, out_specs=P("chan"), check_vma=False)
```

```python
import functools

import jax
import jax.numpy as jnp
from jax import lax
from jax.experimental import pallas as pl
from jax.experimental.pallas import tpu as pltpu
from jax.sharding import PartitionSpec as P

LANES = 128
VMEM_LIMIT = 6 * 2**20
CHIPS = (
    10, 26, 25, 9, 13, 12, 8, 24, 28, 29, 30, 14, 15, 31, 27, 11,
    7, 3, 19, 18, 17, 21, 5, 4, 20, 16, 0, 1, 2, 6, 22, 23,
    39, 35, 34, 38, 54, 55, 51, 50, 49, 53, 52, 48, 32, 33, 37, 36,
    40, 56, 60, 44, 45, 61, 57, 41, 42, 46, 47, 43, 59, 63, 62, 58,
)
LEAD = 56


def sublanes():
    return lax.broadcasted_iota(jnp.int32, (8, LANES), 0)


def moved(upper, amount):
    lane = lax.broadcasted_iota(jnp.int32, (8, LANES), 1)
    turned = pltpu.roll(upper, (LANES - amount) & (LANES - 1), axis=1)
    return jnp.where(lane < LANES - amount, turned, pltpu.roll(turned, 7, axis=0))


def tree(offs_ref, get, total, a_ref, b_ref):
    half = total // 2
    step = jnp.full((8, LANES), offs_ref[2], jnp.int32) > 0
    for q in range(half // 2):
        lower, upper = get(q, 0), get(q, 1)
        by_one = moved(upper, 1)
        b_ref[2 * q] = lower + jnp.where(step, by_one, upper)
        b_ref[2 * q + 1] = lower + by_one
    src, dst = b_ref, a_ref
    length = 2
    while length < half:
        for p in range(length):
            amounts = [offs_ref[2 * length + 2 * p + odd] for odd in range(2)]
            for b in range(half // (2 * length)):
                lower = src[2 * b * length + p]
                upper = src[(2 * b + 1) * length + p]
                for odd in range(2):
                    dst[b * 2 * length + 2 * p + odd] = lower + moved(upper, amounts[odd])
        src, dst = dst, src
        length *= 2
    first = sublanes() < 4
    best = [jnp.full((8, LANES), -jnp.inf, jnp.float32) for _ in range(4)]
    for p in range(half):
        both = src[p]
        other = pltpu.roll(both, 4, axis=0)
        lower = jnp.where(first, both, other)
        even = moved(other, offs_ref[2 * length + 2 * p])
        odd = moved(both, offs_ref[2 * length + 2 * p + 1])
        best[p % 4] = jnp.maximum(best[p % 4], lower + jnp.where(first, even, odd))
    peak = functools.reduce(jnp.maximum, best)
    return jnp.maximum(peak, pltpu.roll(peak, 4, axis=0))


def near_kernel(total, spot, table_ref, main_ref, out_ref, offs_ref, a_ref, b_ref, sem):
    half = total // 4
    copy = pltpu.make_async_copy(table_ref, offs_ref, sem)
    copy.start()
    copy.wait()

    def get(t, r):
        one = main_ref[pl.ds(spot[t] * 8 + r, 4, stride=2), :]
        two = main_ref[pl.ds(spot[t + half] * 8 + r, 4, stride=2), :]
        return jnp.concatenate([one, two], axis=0)

    out_ref[...] = tree(offs_ref, get, total, a_ref, b_ref)


def far_kernel(total, copies, spot, offs_ref, more_ref, main_ref, halo_ref, near_ref, out_ref, a_ref, b_ref):
    half = total // 4
    sub = sublanes()
    keep = (sub % 4 < 2) | (more_ref[0] > 0)

    def get(t, r):
        one, two = spot[t], spot[t + half]
        head_one = main_ref[pl.ds(one * 8 + r + 4, 2, stride=2), :]
        head_two = main_ref[pl.ds(two * 8 + r + 4, 2, stride=2), :]
        tail_one = halo_ref[pl.ds(3 * half * r + one, 2, stride=half), :]
        tail_two = halo_ref[pl.ds(3 * half * r + two, 2, stride=half), :]
        both = jnp.concatenate([head_one, tail_one, head_two, tail_two], axis=0)
        return jnp.where(keep, both, 0.0)

    far = tree(offs_ref, get, total, a_ref, b_ref)
    both = jnp.where(sub % 4 < 2, near_ref[...], pltpu.roll(far, 2, axis=0))
    for k in range(copies // 2):
        out_ref[pl.ds(k * 8, 8), :] = both


def walk(count):
    assert count == 2 * len(CHIPS)
    return [2 * chip + core for chip in CHIPS for core in range(2)]


def to_previous(order, groups):
    place = [t * groups + g for g in range(groups) for t in order]
    return list(zip(place, place[-1:] + place[:-1]))


def local(spectrum, offsets):
    rows, span = spectrum.shape
    count = lax.axis_size("tm")
    groups = lax.axis_size("chan")
    total = rows * count
    cols = span // count // LANES
    order = walk(count)
    spot = [order.index(t) for t in range(count)]
    more = (lax.axis_index("tm") != order[-1]) | (lax.axis_index("chan") != groups - 1)
    more = jnp.reshape(more, (1,)).astype(jnp.int32)
    tiles = spectrum.reshape(rows, span // LANES, LANES).transpose(1, 0, 2)
    main = lax.all_to_all(tiles, "tm", 0, 0, axis_index_groups=[order], tiled=True)
    early = count // 2
    assert max(order[:early]) < early
    window = main.reshape(count, cols, rows, LANES)
    edge = jnp.concatenate([window[:, 0], window[early:, 1]], axis=0)
    halo = lax.ppermute(edge, ("tm", "chan"), to_previous(order, groups))
    main = main.reshape(-1, LANES)
    smem = pl.BlockSpec(memory_space=pltpu.SMEM)
    vmem = pl.BlockSpec(memory_space=pltpu.VMEM)
    scratch = [pltpu.VMEM((total // 2, 8, LANES), jnp.float32)] * 2
    params = pltpu.CompilerParams(vmem_limit_bytes=VMEM_LIMIT)
    cost = pl.CostEstimate(flops=20_000_000, bytes_accessed=600_000, transcendentals=0)
    near, table = pl.pallas_call(
        functools.partial(near_kernel, total, spot),
        out_shape=(jax.ShapeDtypeStruct((8, LANES), jnp.float32), pltpu.SMEM(offsets.shape, jnp.int32)),
        in_specs=[pl.BlockSpec(memory_space=pl.ANY), vmem],
        out_specs=(vmem, smem),
        scratch_shapes=scratch + [pltpu.SemaphoreType.DMA],
        compiler_params=params,
        cost_estimate=cost,
    )(offsets, main)
    best = pl.pallas_call(
        functools.partial(far_kernel, total, count // 2, spot),
        out_shape=jax.ShapeDtypeStruct((count // 2 * cols, LANES), jnp.float32),
        in_specs=[smem, smem, vmem, vmem, vmem],
        out_specs=vmem,
        scratch_shapes=scratch,
        compiler_params=params,
        cost_estimate=cost,
    )(table, more, main, halo.transpose(1, 0, 2).reshape(-1, LANES), near)
    turned = order[2 * LEAD :] + order[: 2 * LEAD]
    cores = [turned[core::2] for core in range(2)]
    ours = lax.all_to_all(best, "tm", 0, 0, axis_index_groups=cores, tiled=True)
    theirs = lax.ppermute(ours, "tm", [(t, t ^ 1) for t in range(count)])
    pair = [part.reshape(count // 2, 1, cols, LANES) for part in (ours, theirs)]
    second = lax.axis_index("tm") % 2 == 1
    first_core = jnp.where(second, pair[1], pair[0])
    second_core = jnp.where(second, pair[0], pair[1])
    both = jnp.concatenate([first_core, second_core], axis=1)
    return jnp.roll(both, LEAD, axis=0).reshape(span)


def solution(mesh):
    placed = (P("tm", "chan"), P())
    return jax.shard_map(local, mesh=mesh, in_specs=placed, out_specs=P("chan"), check_vma=False)
```

```python
import functools

import jax
import jax.numpy as jnp
from jax import lax
from jax.experimental import pallas as pl
from jax.experimental.pallas import tpu as pltpu
from jax.sharding import PartitionSpec as P

LANES = 128
VMEM_LIMIT = 6 * 2**20
CHIPS = (
    10, 11, 15, 31, 27, 23, 19, 18, 2, 3, 7, 6, 22, 26, 30, 14,
    13, 12, 8, 4, 0, 16, 20, 24, 28, 29, 25, 9, 5, 1, 17, 21,
    37, 33, 49, 53, 52, 48, 32, 36, 40, 56, 60, 44, 45, 61, 62, 63,
    59, 55, 51, 35, 34, 50, 54, 38, 39, 43, 47, 46, 42, 41, 57, 58,
)
LEAD = 60


def sublanes():
    return lax.broadcasted_iota(jnp.int32, (8, LANES), 0)


def moved(upper, amount):
    lane = lax.broadcasted_iota(jnp.int32, (8, LANES), 1)
    turned = pltpu.roll(upper, (LANES - amount) & (LANES - 1), axis=1)
    return jnp.where(lane < LANES - amount, turned, pltpu.roll(turned, 7, axis=0))


def tree(offs_ref, get, total, a_ref, b_ref):
    half = total // 2
    step = jnp.full((8, LANES), offs_ref[2], jnp.int32) > 0
    for q in range(half // 2):
        lower, upper = get(q, 0), get(q, 1)
        by_one = moved(upper, 1)
        b_ref[2 * q] = lower + jnp.where(step, by_one, upper)
        b_ref[2 * q + 1] = lower + by_one
    src, dst = b_ref, a_ref
    length = 2
    while length < half:
        for p in range(length):
            amounts = [offs_ref[2 * length + 2 * p + odd] for odd in range(2)]
            for b in range(half // (2 * length)):
                lower = src[2 * b * length + p]
                upper = src[(2 * b + 1) * length + p]
                for odd in range(2):
                    dst[b * 2 * length + 2 * p + odd] = lower + moved(upper, amounts[odd])
        src, dst = dst, src
        length *= 2
    first = sublanes() < 4
    best = [jnp.full((8, LANES), -jnp.inf, jnp.float32) for _ in range(4)]
    for p in range(half):
        both = src[p]
        other = pltpu.roll(both, 4, axis=0)
        lower = jnp.where(first, both, other)
        even = moved(other, offs_ref[2 * length + 2 * p])
        odd = moved(both, offs_ref[2 * length + 2 * p + 1])
        best[p % 4] = jnp.maximum(best[p % 4], lower + jnp.where(first, even, odd))
    peak = functools.reduce(jnp.maximum, best)
    return jnp.maximum(peak, pltpu.roll(peak, 4, axis=0))


def near_kernel(total, spot, table_ref, main_ref, out_ref, offs_ref, a_ref, b_ref, sem):
    half = total // 4
    copy = pltpu.make_async_copy(table_ref, offs_ref, sem)
    copy.start()
    copy.wait()

    def get(t, r):
        one = main_ref[pl.ds(spot[t] * 8 + r, 4, stride=2), :]
        two = main_ref[pl.ds(spot[t + half] * 8 + r, 4, stride=2), :]
        return jnp.concatenate([one, two], axis=0)

    out_ref[...] = tree(offs_ref, get, total, a_ref, b_ref)


def far_kernel(total, copies, spot, offs_ref, more_ref, main_ref, halo_ref, near_ref, out_ref, a_ref, b_ref):
    half = total // 4
    sub = sublanes()
    keep = (sub % 4 < 2) | (more_ref[0] > 0)

    def get(t, r):
        one, two = spot[t], spot[t + half]
        head_one = main_ref[pl.ds(one * 8 + r + 4, 2, stride=2), :]
        head_two = main_ref[pl.ds(two * 8 + r + 4, 2, stride=2), :]
        tail_one = halo_ref[pl.ds(3 * half * r + one, 2, stride=half), :]
        tail_two = halo_ref[pl.ds(3 * half * r + two, 2, stride=half), :]
        both = jnp.concatenate([head_one, tail_one, head_two, tail_two], axis=0)
        return jnp.where(keep, both, 0.0)

    far = tree(offs_ref, get, total, a_ref, b_ref)
    both = jnp.where(sub % 4 < 2, near_ref[...], pltpu.roll(far, 2, axis=0))
    for k in range(copies // 2):
        out_ref[pl.ds(k * 8, 8), :] = both


def walk(count):
    assert count == 2 * len(CHIPS)
    return [2 * chip + core for chip in CHIPS for core in range(2)]


def to_previous(order, groups):
    place = [t * groups + g for g in range(groups) for t in order]
    return list(zip(place, place[-1:] + place[:-1]))


def local(spectrum, offsets):
    rows, span = spectrum.shape
    count = lax.axis_size("tm")
    groups = lax.axis_size("chan")
    total = rows * count
    cols = span // count // LANES
    order = walk(count)
    spot = [order.index(t) for t in range(count)]
    more = (lax.axis_index("tm") != order[-1]) | (lax.axis_index("chan") != groups - 1)
    more = jnp.reshape(more, (1,)).astype(jnp.int32)
    tiles = spectrum.reshape(rows, span // LANES, LANES).transpose(1, 0, 2)
    main = lax.all_to_all(tiles, "tm", 0, 0, axis_index_groups=[order], tiled=True)
    early = count // 2
    assert max(order[:early]) < early
    window = main.reshape(count, cols, rows, LANES)
    edge = jnp.concatenate([window[:, 0], window[early:, 1]], axis=0)
    halo = lax.ppermute(edge, ("tm", "chan"), to_previous(order, groups))
    main = main.reshape(-1, LANES)
    smem = pl.BlockSpec(memory_space=pltpu.SMEM)
    vmem = pl.BlockSpec(memory_space=pltpu.VMEM)
    scratch = [pltpu.VMEM((total // 2, 8, LANES), jnp.float32)] * 2
    params = pltpu.CompilerParams(vmem_limit_bytes=VMEM_LIMIT)
    cost = pl.CostEstimate(flops=20_000_000, bytes_accessed=600_000, transcendentals=0)
    near, table = pl.pallas_call(
        functools.partial(near_kernel, total, spot),
        out_shape=(jax.ShapeDtypeStruct((8, LANES), jnp.float32), pltpu.SMEM(offsets.shape, jnp.int32)),
        in_specs=[pl.BlockSpec(memory_space=pl.ANY), vmem],
        out_specs=(vmem, smem),
        scratch_shapes=scratch + [pltpu.SemaphoreType.DMA],
        compiler_params=params,
        cost_estimate=cost,
    )(offsets, main)
    best = pl.pallas_call(
        functools.partial(far_kernel, total, count // 2, spot),
        out_shape=jax.ShapeDtypeStruct((count // 2 * cols, LANES), jnp.float32),
        in_specs=[smem, smem, vmem, vmem, vmem],
        out_specs=vmem,
        scratch_shapes=scratch,
        compiler_params=params,
        cost_estimate=cost,
    )(table, more, main, halo.transpose(1, 0, 2).reshape(-1, LANES), near)
    turned = order[2 * LEAD :] + order[: 2 * LEAD]
    cores = [turned[core::2] for core in range(2)]
    ours = lax.all_to_all(best, "tm", 0, 0, axis_index_groups=cores, tiled=True)
    theirs = lax.ppermute(ours, "tm", [(t, t ^ 1) for t in range(count)])
    pair = [part.reshape(count // 2, 1, cols, LANES) for part in (ours, theirs)]
    second = lax.axis_index("tm") % 2 == 1
    first_core = jnp.where(second, pair[1], pair[0])
    second_core = jnp.where(second, pair[0], pair[1])
    both = jnp.concatenate([first_core, second_core], axis=1)
    return jnp.roll(both, LEAD, axis=0).reshape(span)


def solution(mesh):
    placed = (P("tm", "chan"), P())
    return jax.shard_map(local, mesh=mesh, in_specs=placed, out_specs=P("chan"), check_vma=False)
```
